128 devices in a mesh: hp: 4 (over x), cp: 32 (over z, y, core).
Axes of the slice: x: 4, y: 4, z: 4, core: 2. Of those that a mesh axis runs over, the one named last changes fastest.
Arguments:
- q: bfloat16 [1, 16384, 32, 128], P(None, ('cp', 'hp'))
- k: bfloat16 [1, 16384, 32, 128], P(None, ('cp', 'hp'))
- v: bfloat16 [1, 16384, 32, 128], P(None, ('cp', 'hp'))
- o: bfloat16 [1, 16384, 32, 128], P(None, ('cp', 'hp'))
- do: bfloat16 [1, 16384, 32, 128], P(None, ('cp', 'hp'))
- lse: float32 [1, 32, 16384], P(None, None, ('cp', 'hp'))
Outputs:
- output 1: bfloat16 [1, 16384, 32, 128], P(None, ('cp', 'hp'))
- output 2: bfloat16 [1, 16384, 32, 128], P(None, ('cp', 'hp'))
- output 3: bfloat16 [1, 16384, 32, 128], P(None, ('cp', 'hp'))
All inputs are finite; a program needn't handle non-finite values.
Results may differ from the reference program's by a relative error of at most 0.001.
Values are sent between devices in bfloat16 or wider.
A program may use at most 1 GiB of HBM per device.

```python
import jax
import jax.numpy as jnp
from jax import lax

B = 1
CHUNK = 256
HKV = 32
GROUP = 1
HEAD = 128
CP = 32

HQ = HKV * GROUP
S = 2 * CP * CHUNK
QB = min(CHUNK, 256)


def _positions():
    c = jnp.arange(2 * CP)
    t = jnp.where(c % 2 == 0, c // 2, 2 * CP - 1 - c // 2)
    return (t[:, None] * CHUNK + jnp.arange(CHUNK)[None, :]).reshape(-1)


def _split_q(x):
    return x.reshape(B, S, HKV, GROUP, HEAD).transpose(0, 2, 3, 1, 4).reshape(B * HKV, GROUP, S, HEAD)


def _split_kv(x):
    return x.transpose(0, 2, 1, 3).reshape(B * HKV, S, HEAD)


def _merge_q(x):
    return x.reshape(B, HKV, GROUP, S, HEAD).transpose(0, 3, 1, 2, 4).reshape(B, S, HQ, HEAD)


def _forward(q, k, v):
    pos = _positions()
    scale = HEAD ** -0.5

    def one(args):
        qh, kh, vh = args
        kf = kh.astype(jnp.float32)
        vf = vh.astype(jnp.float32)

        def body(_, c):
            qc = lax.dynamic_slice_in_dim(qh, c * QB, QB, axis=1).astype(jnp.float32)
            pc = lax.dynamic_slice_in_dim(pos, c * QB, QB)
            s = jnp.einsum('gqd,kd->gqk', qc, kf) * scale
            s = jnp.where(pos[None, :] <= pc[:, None], s, -jnp.inf)
            m = jnp.max(s, axis=-1, keepdims=True)
            e = jnp.exp(s - m)
            l = jnp.sum(e, axis=-1, keepdims=True)
            oc = jnp.einsum('gqk,kd->gqd', e / l, vf)
            return None, (oc, (m + jnp.log(l))[..., 0])

        _, (oc, lc) = lax.scan(body, None, jnp.arange(S // QB))
        return oc.transpose(1, 0, 2, 3).reshape(GROUP, S, HEAD), lc.transpose(1, 0, 2).reshape(GROUP, S)

    o, lse = lax.map(one, (_split_q(q), _split_kv(k), _split_kv(v)))
    return _merge_q(o).astype(jnp.bfloat16), lse.reshape(B, HQ, S)


def setup_inputs(seed: int = 0) -> dict:
    kq, kk, kv, kd = jax.random.split(jax.random.PRNGKey(seed), 4)
    q = jax.random.normal(kq, (B, S, HQ, HEAD), jnp.float32).astype(jnp.bfloat16)
    k = jax.random.normal(kk, (B, S, HKV, HEAD), jnp.float32).astype(jnp.bfloat16)
    v = jax.random.normal(kv, (B, S, HKV, HEAD), jnp.float32).astype(jnp.bfloat16)
    do = (jax.random.normal(kd, (B, S, HQ, HEAD), jnp.float32) * (S ** 0.5 / 8)).astype(jnp.bfloat16)
    o, lse = _forward(q, k, v)
    return {'q': q, 'k': k, 'v': v, 'o': o, 'do': do, 'lse': lse}


def reference(q, k, v, o, do, lse):
    pos = _positions()
    scale = HEAD ** -0.5
    dlt = jnp.sum(do.astype(jnp.float32) * o.astype(jnp.float32), axis=-1)
    dlt = dlt.reshape(B, S, HKV, GROUP).transpose(0, 2, 3, 1).reshape(B * HKV, GROUP, S)

    def one(args):
        qh, kh, vh, doh, lh, eh = args
        kf = kh.astype(jnp.float32)
        vf = vh.astype(jnp.float32)

        def body(carry, c):
            dk, dv = carry
            qc = lax.dynamic_slice_in_dim(qh, c * QB, QB, axis=1).astype(jnp.float32)
            dc = lax.dynamic_slice_in_dim(doh, c * QB, QB, axis=1).astype(jnp.float32)
            lc = lax.dynamic_slice_in_dim(lh, c * QB, QB, axis=1)
            ec = lax.dynamic_slice_in_dim(eh, c * QB, QB, axis=1)
            pc = lax.dynamic_slice_in_dim(pos, c * QB, QB)
            s = jnp.einsum('gqd,kd->gqk', qc, kf) * scale
            p = jnp.where(pos[None, :] <= pc[:, None], jnp.exp(s - lc[..., None]), 0.0)
            dv = dv + jnp.einsum('gqk,gqd->kd', p.astype(jnp.bfloat16).astype(jnp.float32), dc)
            dp = jnp.einsum('gqd,kd->gqk', dc, vf)
            ds = (p * (dp - ec[..., None])).astype(jnp.bfloat16).astype(jnp.float32)
            dq = jnp.einsum('gqk,kd->gqd', ds, kf) * scale
            dk = dk + jnp.einsum('gqk,gqd->kd', ds, qc) * scale
            return (dk, dv), dq

        zero = jnp.zeros((S, HEAD), jnp.float32)
        (dk, dv), dq = lax.scan(body, (zero, zero), jnp.arange(S // QB))
        return dq.transpose(1, 0, 2, 3).reshape(GROUP, S, HEAD), dk, dv

    dq, dk, dv = lax.map(one, (_split_q(q), _split_kv(k), _split_kv(v), _split_q(do), lse.reshape(B * HKV, GROUP, S), dlt))
    dk = dk.reshape(B, HKV, S, HEAD).transpose(0, 2, 1, 3)
    dv = dv.reshape(B, HKV, S, HEAD).transpose(0, 2, 1, 3)
    return _merge_q(dq).astype(jnp.bfloat16), dk.astype(jnp.bfloat16), dv.astype(jnp.bfloat16)
```

```python
import functools

import jax
import jax.numpy as jnp
from jax import lax
from jax.experimental import pallas as pl
from jax.experimental.pallas import tpu as pltpu
from jax.sharding import Mesh, PartitionSpec as P

LOG2E = 1.4426950408889634
BT = 512


def _attn_kernel(scale, n, info, q, do, qt, dot, k, kt, vt, lse, dlt, dq, dkt, dvt, p_s, ds_s, lse_b, dlt_b):
    core, half = info[0], info[1]
    f32, bf16 = jnp.float32, jnp.bfloat16
    dkt[...] = jnp.zeros_like(dkt)
    dvt[...] = jnp.zeros_like(dvt)
    dq[...] = jnp.zeros_like(dq)

    def rows(i):
        return pl.ds(pl.multiple_of(i * BT, BT), BT)

    def stage1(qb, kb, slot, diag):
        qs, ks = rows(qb), rows(kb)
        s = jnp.dot(q[qs, :], kt[:, ks], preferred_element_type=f32)
        dp = jnp.dot(do[qs, :], vt[:, ks], preferred_element_type=f32)
        lb = jnp.tile(lse_b[...], (1, BT // 128))
        db = jnp.tile(dlt_b[...], (1, BT // 128))
        p = jnp.exp2(s * (scale * LOG2E) - lb)
        if diag:
            hi = (2 * qb >= n).astype(jnp.int32)
            r = lax.broadcasted_iota(jnp.int32, (BT, BT), 0)
            c = lax.broadcasted_iota(jnp.int32, (BT, BT), 1)
            e = jnp.where(hi == 1, 1 - core, core)
            qp = (r // 256 * 2 + e) * 256 + r % 256
            jj = c // 128 % 2
            kp = (c // 256 * 2 + jnp.where(hi == 1, 1 - jj, jj)) * 256 + half * 128 + c % 128
            p = jnp.where(kp <= qp, p, 0.0)
        p_s[slot] = p.astype(bf16)
        ds_s[slot] = (p * (dp - db)).astype(bf16)

    def stage2(qb, kb, slot):
        qs, ks = rows(qb), rows(kb)
        dvt[:, ks] += jnp.dot(dot[:, qs], p_s[slot], preferred_element_type=f32)
        dkt[:, ks] += jnp.dot(qt[:, qs], ds_s[slot], preferred_element_type=f32)
        dq[qs, :] += jnp.dot(ds_s[slot], k[ks, :], preferred_element_type=f32)

    def stats(qb):
        qs = rows(qb)
        lse_b[...] = jnp.broadcast_to(lse[:, qs] * LOG2E, (128, BT)).T
        dlt_b[...] = jnp.broadcast_to(dlt[:, qs], (128, BT)).T

    def row(qb, carry):
        stats(qb)

        def full(kb, carry):
            pq, pk, slot = carry
            stage2(pq, pk, 1 - slot)
            stage1(qb, kb, slot, False)
            return qb, kb, 1 - slot

        pq, pk, slot = lax.fori_loop(0, qb, full, carry)
        stage2(pq, pk, 1 - slot)
        stage1(qb, qb, slot, True)
        return qb, qb, 1 - slot

    p_s[1] = jnp.zeros((BT, BT), bf16)
    ds_s[1] = jnp.zeros((BT, BT), bf16)
    pq, pk, slot = lax.fori_loop(0, n, row, (0, 0, 0))
    stage2(pq, pk, 1 - slot)


def _attention(q, do, k, v, lse, dlt, core, half, scale):
    t, d = q.shape
    info = jnp.stack([core, half]).astype(jnp.int32)
    f32 = jnp.float32
    vm = pl.BlockSpec(memory_space=pltpu.VMEM)
    return pl.pallas_call(
        functools.partial(_attn_kernel, scale, t // BT),
        out_shape=(jax.ShapeDtypeStruct((t, d), f32), jax.ShapeDtypeStruct((d, t), f32), jax.ShapeDtypeStruct((d, t), f32)),
        in_specs=[pl.BlockSpec(memory_space=pltpu.SMEM)] + [vm] * 9,
        out_specs=(vm, vm, vm),
        scratch_shapes=[
            pltpu.VMEM((2, BT, BT), jnp.bfloat16),
            pltpu.VMEM((2, BT, BT), jnp.bfloat16),
            pltpu.VMEM((BT, 128), f32),
            pltpu.VMEM((BT, 128), f32),
        ],
        compiler_params=pltpu.CompilerParams(vmem_limit_bytes=62 * 1024 * 1024),
        cost_estimate=pl.CostEstimate(flops=5 * t * t * d, bytes_accessed=26 * t * d, transcendentals=t * t // 2),
        name='attn_bwd',
    )(info, q, do, q.T, do.T, k, k.T, v.T, lse, dlt)


def solution(mesh):
    x, cp = mesh.devices.shape
    fine = Mesh(mesh.devices.reshape(2, 2, 4, 4, 2), ('xa', 'xb', 'z', 'y', 'core'))
    rows = ('z', 'y', 'core', 'xa', 'xb')
    seq = P(None, rows, None, None)
    stat = P(None, None, rows)
    heads = ('z', 'y', 'xa')

    def body(q, k, v, o, do, lse):
        _, r, h, d = q.shape
        f32 = jnp.float32
        scale = d ** -0.5
        core, half = lax.axis_index('core'), lax.axis_index('xb')
        dlt = jnp.sum(do.astype(f32) * o.astype(f32), axis=-1)[0].T
        st = jnp.stack([lse[0], dlt], axis=1)
        kv = jnp.stack([k[0], v[0]]).transpose(2, 0, 1, 3)
        qd = jnp.stack([q[0], do[0]]).transpose(2, 0, 1, 3)
        kv, qd, st = [lax.all_to_all(a, heads, 0, 0, tiled=True) for a in (kv, qd, st)]

        def order(a):
            a = a.reshape(16, 2, *a.shape[1:])
            return jnp.concatenate([a[:, 0], a[::-1, 1]], axis=0)

        kv, qd, st = order(kv), order(qd), order(st)
        kv = lax.all_gather(kv, 'core', axis=2)
        qd = lax.all_gather(qd, 'xb', axis=2)
        st = lax.all_gather(st, 'xb', axis=2)
        t = 64 * r
        kk, vv = [kv[:, i].reshape(t, d) for i in range(2)]
        qq, dd = [qd[:, i].reshape(t, d) for i in range(2)]
        ll, dl = [st[:, i].reshape(1, t) for i in range(2)]
        dq, dkt, dvt = _attention(qq, dd, kk, vv, ll, dl, core, half, scale)

        def swap(a, axis):
            i = lax.axis_index(axis)
            mine = lax.dynamic_index_in_dim(a, i, 1, keepdims=False)
            other = lax.dynamic_index_in_dim(a, 1 - i, 1, keepdims=False)
            return mine + lax.ppermute(other, axis, [(0, 1), (1, 0)])

        dq = swap(dq.reshape(32, 2, r, d), 'xb')
        dk = swap(dkt.T.reshape(32, 2, r, d), 'core')
        dv = swap(dvt.T.reshape(32, 2, r, d), 'core')
        out = jnp.stack([dq * scale, dk * scale, dv], axis=1).astype(jnp.bfloat16)
        out = jnp.stack([out[:16], out[16:][::-1]], axis=1).reshape(32, 3, r, d)
        out = lax.all_to_all(out, heads, 0, 0, tiled=True)
        out = out.transpose(1, 2, 0, 3)
        return out[0][None], out[1][None], out[2][None]

    return jax.shard_map(body, mesh=fine, in_specs=(seq, seq, seq, seq, seq, stat), out_specs=(seq, seq, seq), check_vma=False)
```

```python
import functools

import jax
import jax.numpy as jnp
from jax import lax
from jax.experimental import pallas as pl
from jax.experimental.pallas import tpu as pltpu
from jax.sharding import Mesh, PartitionSpec as P

LOG2E = 1.4426950408889634
AXES = ('x1', 'x0', 'zh', 'zl', 'yh', 'yl', 'core')
N = 16
NA = 12
AHEAD = 2


def _kernel(scale, x4, st, out, qd, kv, qdt, kvt, sb, stb, dq, dkt, dvt, p_s, ds_s, dq_rx, dk_rx, dv_rx, stage, send, recv_qd, recv_kv, recv_st, fwd_send, fwd_qd, fwd_kv, fwd_st, x_send, x_dq, x_dk, x_dv, o_send, o_recv):
    f32, bf16 = jnp.float32, jnp.bfloat16
    R, D = x4.shape[2], x4.shape[3]
    BT = 4 * R
    x1, x0, zh, zl, yh, yl, core = [lax.axis_index(a) for a in AXES]
    xb = (x0 + x1) % 2

    def source(m):
        tx, ty, tzl, tzh = m % 2, m // 2 % 2, m // 4 % 2, m // 8
        sx = (x1 + tx) % 2
        return sx, (sx + xb) % 2, (zh + tzh) % 2, (zl + tzl) % 2, (yh + ty) % 2

    def device(m, u):
        sx, sx0, szh, szl, syh = source(m)
        return (sx, sx0, szh, szl, syh, (yl + u) % 2, core)

    def block(sx, syl):
        return syl + sx * (1 - 2 * syl)

    def place(m):
        sx, _, szh, szl, syh = source(m)
        zzy = 4 * szh + 2 * szl + syh
        return zzy + sx * (N - 1 - 2 * zzy)

    def head(dev):
        dx, _, dzh, dzl, dyh, dyl, _ = dev
        return (((dzh * 2 + dzl) * 2 + dyh) * 2 + dyl) * 2 + dx

    def chunk(m, b, i):
        return pl.ds(pl.multiple_of(m * BT + b * 2 * R + i * R, R), R)

    me = (x1, x0, zh, zl, yh, yl, core)
    x_peer = (x1, 1 - x0, zh, zl, yh, yl, core)
    c_peer = (x1, x0, zh, zl, yh, yl, 1 - core)
    my_b = block(x1, yl)

    def remote(src, dst, s_sem, r_sem, dev):
        return pltpu.make_async_remote_copy(src_ref=src, dst_ref=dst, send_sem=s_sem, recv_sem=r_sem, device_id=dev, device_id_type=pl.DeviceIdType.MESH)

    barrier = pltpu.get_barrier_semaphore()

    @pl.loop(1, 2 * N)
    def _(t):
        pl.semaphore_signal(barrier, inc=1, device_id=device(t // 2, t % 2), device_id_type=pl.DeviceIdType.MESH)

    for dev in (x_peer, c_peer):
        pl.semaphore_signal(barrier, inc=1, device_id=dev, device_id_type=pl.DeviceIdType.MESH)
    pl.semaphore_wait(barrier, 2 * N + 1)

    def parts(h, m, t):
        return (
            (x4.at[h, pl.ds(0, 2)], qd.at[:, chunk(m, my_b, x0)], send.at[0], recv_qd.at[t]),
            (x4.at[h, pl.ds(2, 2)], kv.at[:, chunk(m, my_b, core)], send.at[1], recv_kv.at[t]),
            (st.at[h], sb.at[:, chunk(m, my_b, x0)], send.at[2], recv_st.at[t]),
        )

    for src, dst, _, sem in parts(head(me), 0, 0):
        pltpu.make_async_copy(src, dst, sem).start()

    @pl.loop(1, 2 * N)
    def _(t):
        dev = device(t // 2, t % 2)
        for src, dst, ss, rs in parts(head(dev), t // 2, t):
            remote(src, dst, ss, rs, dev).start()

    def direct(m, u):
        sx, sx0, *_ = source(m)
        b = block(sx, (yl + u) % 2)
        return qd.at[:, chunk(m, b, sx0)], kv.at[:, chunk(m, b, core)], sb.at[:, chunk(m, b, sx0)]

    def passed(m, u):
        sx, sx0, *_ = source(m)
        b = block(sx, (yl + u) % 2)
        return qd.at[:, chunk(m, b, 1 - sx0)], kv.at[:, chunk(m, b, 1 - core)], sb.at[:, chunk(m, b, 1 - sx0)]

    def arrive(m):
        for u in range(2):
            t = 2 * m + u
            a, b, c = direct(m, u)
            pltpu.make_async_copy(a, a, recv_qd.at[t]).wait()
            remote(a, a, fwd_send.at[0], fwd_qd.at[t], x_peer).start()
            pltpu.make_async_copy(b, b, recv_kv.at[t]).wait()
            remote(b, b, fwd_send.at[1], fwd_kv.at[t], c_peer).start()
            pltpu.make_async_copy(c, c, recv_st.at[t]).wait()
            remote(c, c, fwd_send.at[2], fwd_st.at[t], x_peer).start()

    def rows(i):
        return pl.ds(pl.multiple_of(i * BT, BT), BT)

    def complete(m):
        for u in range(2):
            t = 2 * m + u
            a, b, c = passed(m, u)
            pltpu.make_async_copy(a, a, fwd_qd.at[t]).wait()
            pltpu.make_async_copy(b, b, fwd_kv.at[t]).wait()
            pltpu.make_async_copy(c, c, fwd_st.at[t]).wait()
        rs = rows(m)
        for i in range(2):
            qdt[i, :, rs] = qd[i, rs, :].T
            kvt[i, :, rs] = kv[i, rs, :].T
        stb[0, rs, :] = jnp.broadcast_to(sb[0:1, rs] * LOG2E, (128, BT)).T
        stb[1, rs, :] = jnp.broadcast_to(sb[1:2, rs], (128, BT)).T

    dkt[...] = jnp.zeros_like(dkt)
    dvt[...] = jnp.zeros_like(dvt)
    dq[...] = jnp.zeros_like(dq)
    p_s[1] = jnp.zeros((BT, BT), bf16)
    ds_s[1] = jnp.zeros((BT, BT), bf16)

    def stage1(qb, kb, slot, diag):
        qs, ks = rows(qb), rows(kb)
        s = jnp.dot(qd[0, qs, :], kvt[0, :, ks], preferred_element_type=f32)
        dp = jnp.dot(qd[1, qs, :], kvt[1, :, ks], preferred_element_type=f32)
        lb = jnp.tile(stb[0, qs, :], (1, BT // 128)) if BT >= 128 else stb[0, qs, :BT]
        db = jnp.tile(stb[1, qs, :], (1, BT // 128)) if BT >= 128 else stb[1, qs, :BT]
        p = jnp.exp2(s * (scale * LOG2E) - lb)
        if diag:
            hi = source(qb)[0]
            r = lax.broadcasted_iota(jnp.int32, (BT, BT), 0)
            c = lax.broadcasted_iota(jnp.int32, (BT, BT), 1)
            e = core + hi * (1 - 2 * core)
            qp = (r // (2 * R) * 2 + e) * (2 * R) + r % (2 * R)
            cc = c // R % 2
            half = xb + hi * (1 - 2 * xb)
            kp = (c // (2 * R) * 2 + cc + hi * (1 - 2 * cc)) * (2 * R) + half * R + c % R
            p = jnp.where(kp <= qp, p, 0.0)
        p_s[slot] = p.astype(bf16)
        ds_s[slot] = (p * (dp - db)).astype(bf16)

    def stage2(qb, kb, slot):
        qs, ks = rows(qb), rows(kb)
        dvt[:, ks] += jnp.dot(qdt[1, :, qs], p_s[slot], preferred_element_type=f32)
        dkt[:, ks] += jnp.dot(qdt[0, :, qs], ds_s[slot], preferred_element_type=f32)
        dq[qs, :] += jnp.dot(ds_s[slot], kv[0, ks, :], preferred_element_type=f32)

    def pair(i, j, carry):
        pq, pk, slot = carry
        late = (place(i) > place(j)).astype(jnp.int32)
        qb = j + late * (i - j)
        kb = i + j - qb
        stage2(pq, pk, 1 - slot)
        stage1(qb, kb, slot, False)
        return qb, kb, 1 - slot

    def same(i, carry):
        pq, pk, slot = carry
        stage2(pq, pk, 1 - slot)
        stage1(i, i, slot, True)
        return i, i, 1 - slot

    def swap(m):
        sx, sx0, *_ = source(m)
        for b in range(2):
            w = 2 * m + b
            a = chunk(m, b, 1 - sx0)
            c = chunk(m, b, 1 - core)
            remote(dq.at[a, :], dq_rx.at[w], x_send.at[0], x_dq.at[w], x_peer).start()
            remote(dkt.at[:, c], dk_rx.at[w], x_send.at[1], x_dk.at[w], c_peer).start()
            remote(dvt.at[:, c], dv_rx.at[w], x_send.at[2], x_dv.at[w], c_peer).start()

    def combine(m):
        sx, sx0, *_ = source(m)
        for b in range(2):
            w = 2 * m + b
            pltpu.make_async_copy(dq_rx.at[w], dq_rx.at[w], x_dq.at[w]).wait()
            pltpu.make_async_copy(dk_rx.at[w], dk_rx.at[w], x_dk.at[w]).wait()
            pltpu.make_async_copy(dv_rx.at[w], dv_rx.at[w], x_dv.at[w]).wait()
            a = chunk(m, b, sx0)
            c = chunk(m, b, core)
            stage[w, 0] = ((dq[a, :] + dq_rx[w]) * scale).astype(bf16)
            stage[w, 1] = ((dkt[:, c] + dk_rx[w]) * scale).T.astype(bf16)
            stage[w, 2] = (dvt[:, c] + dv_rx[w]).T.astype(bf16)

    def emit(m):
        sx, sx0, szh, szl, syh = source(m)
        for b in range(2):
            syl = block(sx, b)
            dev = (sx, sx0, szh, szl, syh, syl, core)
            own = jnp.logical_and(m == 0, syl == yl)

            @pl.when(own)
            def _():
                pltpu.make_async_copy(stage.at[2 * m + b], out.at[head(me)], o_send.at[1]).start()

            @pl.when(jnp.logical_not(own))
            def _():
                remote(stage.at[2 * m + b], out.at[head(me)], o_send.at[0], o_recv.at[0], dev).start()

    for m in range(AHEAD):
        arrive(m)

    def inflow(m, carry):
        @pl.when(m + AHEAD < N)
        def _():
            arrive(m + AHEAD)

        complete(m)
        carry = lax.fori_loop(0, m, lambda j, c: pair(m, j, c), carry)
        return same(m, carry)

    carry = lax.fori_loop(0, NA, inflow, (0, 0, 0))

    @pl.loop(NA, N)
    def _(m):
        @pl.when(m + AHEAD < N)
        def _():
            arrive(m + AHEAD)

        complete(m)

    def after(f):
        @pl.when(f >= 1)
        def _():
            swap(f - 1)

        @pl.when(f >= 2)
        def _():
            combine(f - 2)

        @pl.when(f >= 3)
        def _():
            emit(f - 3)

    def outflow(f, carry):
        carry = lax.fori_loop(NA, N, lambda j, c: pair(f, j, c), carry)
        after(f)
        return carry

    carry = lax.fori_loop(0, NA, outflow, carry)

    def last(f, carry):
        carry = same(f, carry)
        carry = lax.fori_loop(f + 1, N, lambda j, c: pair(f, j, c), carry)
        after(f)
        return carry

    pq, pk, slot = lax.fori_loop(NA, N, last, carry)
    stage2(pq, pk, 1 - slot)
    combine(N - 2)
    swap(N - 1)
    emit(N - 3)
    emit(N - 2)
    combine(N - 1)
    emit(N - 1)

    def drain(ref, sem):
        pltpu.make_async_copy(ref, ref, sem).wait()

    drain(x4.at[pl.ds(0, 2 * N - 1), pl.ds(0, 2)], send.at[0])
    drain(x4.at[pl.ds(0, 2 * N - 1), pl.ds(0, 2)], send.at[1])
    drain(st.at[pl.ds(0, 2 * N - 1)], send.at[2])
    drain(x4.at[pl.ds(0, 2 * N), pl.ds(0, 2)], fwd_send.at[0])
    drain(x4.at[pl.ds(0, 2 * N), pl.ds(0, 2)], fwd_send.at[1])
    drain(st.at[pl.ds(0, 2 * N)], fwd_send.at[2])
    drain(dq_rx, x_send.at[0])
    drain(dk_rx, x_send.at[1])
    drain(dv_rx, x_send.at[2])
    drain(stage.at[pl.ds(0, 2 * N - 1)], o_send.at[0])
    drain(stage.at[0], o_send.at[1])
    drain(stage.at[pl.ds(0, 2 * N - 1)], o_recv.at[0])


def _attention(x4, st, scale):
    h, _, r, d = x4.shape
    t = 4 * r * N
    f32, bf16, dma = jnp.float32, jnp.bfloat16, pltpu.SemaphoreType.DMA
    hbm = pl.BlockSpec(memory_space=pl.ANY)
    return pl.pallas_call(
        functools.partial(_kernel, scale),
        out_shape=jax.ShapeDtypeStruct((h, 3, r, d), bf16),
        in_specs=[hbm, hbm],
        out_specs=hbm,
        scratch_shapes=[
            pltpu.VMEM((2, t, d), bf16),
            pltpu.VMEM((2, t, d), bf16),
            pltpu.VMEM((2, d, t), bf16),
            pltpu.VMEM((2, d, t), bf16),
            pltpu.VMEM((2, t), f32),
            pltpu.VMEM((2, t, 128), f32),
            pltpu.VMEM((t, d), f32),
            pltpu.VMEM((d, t), f32),
            pltpu.VMEM((d, t), f32),
            pltpu.VMEM((2, 4 * r, 4 * r), bf16),
            pltpu.VMEM((2, 4 * r, 4 * r), bf16),
            pltpu.VMEM((h, r, d), f32),
            pltpu.VMEM((h, d, r), f32),
            pltpu.VMEM((h, d, r), f32),
            pltpu.VMEM((h, 3, r, d), bf16),
            dma((3,)), dma((h,)), dma((h,)), dma((h,)),
            dma((3,)), dma((h,)), dma((h,)), dma((h,)),
            dma((3,)), dma((h,)), dma((h,)), dma((h,)),
            dma((2,)), dma((1,)),
        ],
        compiler_params=pltpu.CompilerParams(collective_id=0, has_side_effects=True, vmem_limit_bytes=63 * 1024 * 1024),
        name='attn_bwd',
    )(x4, st)


def solution(mesh):
    fine = Mesh(mesh.devices.reshape((2,) * 7), AXES)
    rows = ('zh', 'zl', 'yh', 'yl', 'core', 'x1', 'x0')
    seq = P(None, rows, None, None)
    stat = P(None, None, rows)

    def body(q, k, v, o, do, lse):
        f32 = jnp.float32
        scale = q.shape[3] ** -0.5
        dlt = jnp.sum(do.astype(f32) * o.astype(f32), axis=-1)[0].T
        st = jnp.stack([lse[0], dlt], axis=1)
        x4 = jnp.stack([q[0], do[0], k[0], v[0]]).transpose(2, 0, 1, 3)
        out = _attention(x4, st, scale).transpose(1, 2, 0, 3)
        return out[0][None], out[1][None], out[2][None]

    return jax.shard_map(body, mesh=fine, in_specs=(seq, seq, seq, seq, seq, stat), out_specs=(seq, seq, seq), check_vma=False)
```

```python
import functools

import jax
import jax.numpy as jnp
from jax import lax
from jax.experimental import pallas as pl
from jax.experimental.pallas import tpu as pltpu
from jax.sharding import Mesh, PartitionSpec as P

LOG2E = 1.4426950408889634
AXES = ('x1', 'x0', 'zh', 'zl', 'yh', 'yl', 'core')
N = 16
NA = 10
NF = 5
AHEAD = 1
FIRST = 4


def _kernel(scale, qh, doh, kh, vh, st, out_q, out_k, out_v, qd, kv, qdt, kvt, sb, stb, dq, dkt, dvt, p_s, ds_s, dst_s, dq_rx, dk_rx, dv_rx, stage, send, recv_qd, recv_kv, recv_st, fwd_send, fwd_qd, fwd_kv, fwd_st, x_send, x_dq, x_dk, x_dv, o_send, o_recv):
    f32, bf16 = jnp.float32, jnp.bfloat16
    R = qh.shape[1]
    BT = 4 * R
    x1, x0, zh, zl, yh, yl, core = [lax.axis_index(a) for a in AXES]
    xb = (x0 + x1) % 2

    def source(m):
        a, b, c, d = m % 2, m // 2 % 2, m // 4 % 2, m // 8
        tx, ty, tzl, tzh = (a + b) % 2, (a + c) % 2, d, a
        sx = (x1 + tx) % 2
        return sx, (sx + xb) % 2, (zh + tzh) % 2, (zl + tzl) % 2, (yh + ty) % 2

    def device(m, u):
        sx, sx0, szh, szl, syh = source(m)
        return (sx, sx0, szh, szl, syh, (yl + u) % 2, core)

    def block(sx, syl):
        return syl + sx * (1 - 2 * syl)

    def place(m):
        sx, _, szh, szl, syh = source(m)
        zzy = 4 * szh + 2 * szl + syh
        return zzy + sx * (N - 1 - 2 * zzy)

    def head(dev):
        dx, _, dzh, dzl, dyh, dyl, _ = dev
        return (((dzh * 2 + dzl) * 2 + dyh) * 2 + dyl) * 2 + dx

    def chunk(m, b, i):
        return pl.ds(pl.multiple_of(m * BT + b * 2 * R + i * R, R), R)

    me = (x1, x0, zh, zl, yh, yl, core)
    x_peer = (x1, 1 - x0, zh, zl, yh, yl, core)
    c_peer = (x1, x0, zh, zl, yh, yl, 1 - core)
    my_b = block(x1, yl)

    def remote(src, dst, s_sem, r_sem, dev):
        return pltpu.make_async_remote_copy(src_ref=src, dst_ref=dst, send_sem=s_sem, recv_sem=r_sem, device_id=dev, device_id_type=pl.DeviceIdType.MESH)

    barrier = pltpu.get_barrier_semaphore()

    @pl.loop(1, 2 * N)
    def _(t):
        pl.semaphore_signal(barrier, inc=1, device_id=device(t // 2, t % 2), device_id_type=pl.DeviceIdType.MESH)

    for dev in (x_peer, c_peer):
        pl.semaphore_signal(barrier, inc=1, device_id=dev, device_id_type=pl.DeviceIdType.MESH)
    pl.semaphore_wait(barrier, 2 * N + 1)

    def parts(h, m, t):
        a, b = chunk(m, my_b, x0), chunk(m, my_b, core)
        return (
            (qh.at[h], qd.at[0, a, :], send.at[0], recv_qd.at[t]),
            (doh.at[h], qd.at[1, a, :], send.at[0], recv_qd.at[t]),
            (kh.at[h], kv.at[0, b, :], send.at[1], recv_kv.at[t]),
            (vh.at[h], kv.at[1, b, :], send.at[1], recv_kv.at[t]),
            (st.at[h], sb.at[:, a], send.at[2], recv_st.at[t]),
        )

    for src, dst, _, sem in parts(head(me), 0, 0):
        pltpu.make_async_copy(src, dst, sem).start()

    def issue(m):
        for u in range(2):
            @pl.when(2 * m + u > 0)
            def _():
                dev = device(m, u)
                for src, dst, ss, rs in parts(head(dev), m, 2 * m + u):
                    remote(src, dst, ss, rs, dev).start()

    @pl.loop(0, FIRST)
    def _(m):
        issue(m)

    def direct(m, u):
        sx, sx0, *_ = source(m)
        b = block(sx, (yl + u) % 2)
        return qd.at[:, chunk(m, b, sx0)], kv.at[:, chunk(m, b, core)], sb.at[:, chunk(m, b, sx0)]

    def passed(m, u):
        sx, sx0, *_ = source(m)
        b = block(sx, (yl + u) % 2)
        return qd.at[:, chunk(m, b, 1 - sx0)], kv.at[:, chunk(m, b, 1 - core)], sb.at[:, chunk(m, b, 1 - sx0)]

    def arrive(m):
        for u in range(2):
            t = 2 * m + u
            a, b, c = direct(m, u)
            pltpu.make_async_copy(a, a, recv_qd.at[t]).wait()
            remote(a, a, fwd_send.at[0], fwd_qd.at[t], x_peer).start()
            pltpu.make_async_copy(b, b, recv_kv.at[t]).wait()
            remote(b, b, fwd_send.at[1], fwd_kv.at[t], c_peer).start()
            pltpu.make_async_copy(c, c, recv_st.at[t]).wait()
            remote(c, c, fwd_send.at[2], fwd_st.at[t], x_peer).start()

        @pl.loop(FIRST + 2 * m, FIRST + 2 * m + 2)
        def _(w):
            @pl.when(w < N)
            def _():
                issue(w)

    def rows(i):
        return pl.ds(pl.multiple_of(i * BT, BT), BT)

    def complete(m):
        for u in range(2):
            t = 2 * m + u
            a, b, c = passed(m, u)
            pltpu.make_async_copy(a, a, fwd_qd.at[t]).wait()
            pltpu.make_async_copy(b, b, fwd_kv.at[t]).wait()
            pltpu.make_async_copy(c, c, fwd_st.at[t]).wait()
        rs = rows(m)
        for i in range(2):
            qdt[i, :, rs] = qd[i, rs, :].T
            kvt[i, :, rs] = kv[i, rs, :].T
        stb[0, rs, :] = jnp.broadcast_to(sb[0:1, rs] * LOG2E, (128, BT)).T
        stb[1, rs, :] = jnp.broadcast_to(sb[1:2, rs], (128, BT)).T

    dkt[...] = jnp.zeros_like(dkt)
    dvt[...] = jnp.zeros_like(dvt)
    dq[...] = jnp.zeros_like(dq)
    p_s[1] = jnp.zeros((BT, BT), bf16)
    ds_s[1] = jnp.zeros((BT, BT), bf16)
    dst_s[1] = jnp.zeros((BT, BT), bf16)

    def stage1(qb, kb, slot, diag):
        ks = rows(kb)
        for g in range(2):
            gs = pl.ds(pl.multiple_of(qb * BT + g * 2 * R, 2 * R), 2 * R)
            go = pl.ds(g * 2 * R, 2 * R)
            s = jnp.dot(qd[0, gs, :], kvt[0, :, ks], preferred_element_type=f32)
            dp = jnp.dot(qd[1, gs, :], kvt[1, :, ks], preferred_element_type=f32)
            lb, db = [jnp.tile(stb[i, gs, :], (1, BT // 128)) if BT >= 128 else stb[i, gs, :BT] for i in range(2)]
            p = jnp.exp2(s * (scale * LOG2E) - lb)
            if diag:
                hi = source(qb)[0]
                r = lax.broadcasted_iota(jnp.int32, p.shape, 0)
                c = lax.broadcasted_iota(jnp.int32, p.shape, 1)
                qp = (g * 2 + core + hi * (1 - 2 * core)) * (2 * R) + r
                cc = c // R % 2
                half = xb + hi * (1 - 2 * xb)
                kp = (c // (2 * R) * 2 + cc + hi * (1 - 2 * cc)) * (2 * R) + half * R + c % R
                p = jnp.where(kp <= qp, p, 0.0)
            p_s[slot, go, :] = p.astype(bf16)
            ds = (p * (dp - db)).astype(bf16)
            ds_s[slot, go, :] = ds
            dst_s[slot, :, go] = ds.T

    def stage2(qb, kb, slot):
        qs, ks = rows(qb), rows(kb)
        dvt[:, ks] += jnp.dot(qdt[1, :, qs], p_s[slot], preferred_element_type=f32)
        dkt[:, ks] += jnp.dot(qdt[0, :, qs], ds_s[slot], preferred_element_type=f32)
        dq[:, qs] += jnp.dot(kvt[0, :, ks], dst_s[slot], preferred_element_type=f32)

    def rank(i, j):
        late = (place(i) > place(j)).astype(jnp.int32)
        qb = j + late * (i - j)
        return qb, i + j - qb

    def two(i, j, carry):
        a, b = rank(i, j), rank(i, j + 1)
        stage2(*carry, 1)
        stage1(*a, 0, False)
        stage1(*b, 1, False)
        stage2(*a, 0)
        return b

    def diagonal(i, j, with_pair, carry):
        @pl.when(with_pair)
        def _():
            a = rank(i, j)
            stage2(*carry, 1)
            stage1(*a, 0, False)
            stage1(i, i, 1, True)
            stage2(*a, 0)

        @pl.when(jnp.logical_not(with_pair))
        def _():
            stage2(*carry, 1)
            stage1(i, i, 1, True)

        return i, i

    def swap(m):
        sx, sx0, *_ = source(m)
        for b in range(2):
            w = 2 * m + b
            a = chunk(m, b, 1 - sx0)
            c = chunk(m, b, 1 - core)
            remote(dq.at[:, a], dq_rx.at[w], x_send.at[0], x_dq.at[w], x_peer).start()
            remote(dkt.at[:, c], dk_rx.at[w], x_send.at[1], x_dk.at[w], c_peer).start()
            remote(dvt.at[:, c], dv_rx.at[w], x_send.at[2], x_dv.at[w], c_peer).start()

    def combine(m):
        sx, sx0, *_ = source(m)
        for b in range(2):
            w = 2 * m + b
            pltpu.make_async_copy(dq_rx.at[w], dq_rx.at[w], x_dq.at[w]).wait()
            pltpu.make_async_copy(dk_rx.at[w], dk_rx.at[w], x_dk.at[w]).wait()
            pltpu.make_async_copy(dv_rx.at[w], dv_rx.at[w], x_dv.at[w]).wait()
            a = chunk(m, b, sx0)
            c = chunk(m, b, core)
            stage[w, 0] = ((dq[:, a] + dq_rx[w]) * scale).T.astype(bf16)
            stage[w, 1] = ((dkt[:, c] + dk_rx[w]) * scale).T.astype(bf16)
            stage[w, 2] = (dvt[:, c] + dv_rx[w]).T.astype(bf16)

    def emit(m):
        sx, sx0, szh, szl, syh = source(m)
        for b in range(2):
            syl = block(sx, b)
            dev = (sx, sx0, szh, szl, syh, syl, core)
            own = jnp.logical_and(m == 0, syl == yl)
            ends = [(stage.at[2 * m + b, i], o.at[head(me)]) for i, o in enumerate((out_q, out_k, out_v))]

            @pl.when(own)
            def _():
                for src, dst in ends:
                    pltpu.make_async_copy(src, dst, o_send.at[1]).start()

            @pl.when(jnp.logical_not(own))
            def _():
                for src, dst in ends:
                    remote(src, dst, o_send.at[0], o_recv.at[0], dev).start()

    for m in range(AHEAD):
        arrive(m)

    def inflow(m, carry):
        count = 1 + (m >= NF).astype(jnp.int32)
        first = m + AHEAD + (m - NF) * (count - 1)

        @pl.loop(0, count)
        def _(i):
            @pl.when(first + i < N)
            def _():
                arrive(first + i)

        complete(m)
        carry = diagonal(m, m - 1, m % 2 == 1, carry)
        return lax.fori_loop(0, m // 2, lambda j, c: two(m, 2 * j, c), carry)

    carry = lax.fori_loop(0, NA, inflow, (0, 0))

    @pl.loop(NA, N)
    def _(m):
        complete(m)

    def outflow(f, carry):
        def step(j, carry):
            carry = two(f, NA + 2 * j, carry)

            @pl.when(jnp.logical_and(j == 0, f >= 1))
            def _():
                swap(f - 1)

            @pl.when(jnp.logical_and(j == 1, f >= 2))
            def _():
                combine(f - 2)

            @pl.when(jnp.logical_and(j == 2, f >= 2))
            def _():
                emit(f - 2)

            return carry

        return lax.fori_loop(0, (N - NA) // 2, step, carry)

    carry = lax.fori_loop(0, NA, outflow, carry)

    def last(f, carry):
        carry = diagonal(f, N - 1, f % 2 == 0, carry)
        swap(f - 1)

        @pl.when(f > NA)
        def _():
            emit(f - 3)

        carry = lax.fori_loop(0, (N - 1 - f) // 2, lambda j, c: two(f, f + 1 + 2 * j, c), carry)
        combine(f - 2)
        return carry

    carry = lax.fori_loop(NA, N, last, carry)
    stage2(*carry, 1)
    emit(N - 3)
    swap(N - 1)
    combine(N - 2)
    emit(N - 2)
    combine(N - 1)
    emit(N - 1)

    def drain(ref, sem):
        pltpu.make_async_copy(ref, ref, sem).wait()

    drain(stage.at[pl.ds(0, 2 * N - 1), pl.ds(0, 2)], send.at[0])
    drain(stage.at[pl.ds(0, 2 * N - 1), pl.ds(0, 2)], send.at[1])
    drain(st.at[pl.ds(0, 2 * N - 1)], send.at[2])
    drain(stage.at[pl.ds(0, 2 * N), pl.ds(0, 2)], fwd_send.at[0])
    drain(stage.at[pl.ds(0, 2 * N), pl.ds(0, 2)], fwd_send.at[1])
    drain(st.at[pl.ds(0, 2 * N)], fwd_send.at[2])
    drain(dq_rx, x_send.at[0])
    drain(dk_rx, x_send.at[1])
    drain(dv_rx, x_send.at[2])
    drain(stage.at[pl.ds(0, 2 * N - 1)], o_send.at[0])
    drain(stage.at[0], o_send.at[1])
    drain(stage.at[pl.ds(0, 2 * N - 1)], o_recv.at[0])


def _attention(qh, doh, kh, vh, st, scale):
    h, r, d = qh.shape
    t = 4 * r * N
    f32, bf16, dma = jnp.float32, jnp.bfloat16, pltpu.SemaphoreType.DMA
    hbm = pl.BlockSpec(memory_space=pl.ANY)
    return pl.pallas_call(
        functools.partial(_kernel, scale),
        out_shape=(jax.ShapeDtypeStruct((h, r, d), bf16),) * 3,
        in_specs=[hbm] * 5,
        out_specs=(hbm,) * 3,
        scratch_shapes=[
            pltpu.VMEM((2, t, d), bf16),
            pltpu.VMEM((2, t, d), bf16),
            pltpu.VMEM((2, d, t), bf16),
            pltpu.VMEM((2, d, t), bf16),
            pltpu.VMEM((2, t), f32),
            pltpu.VMEM((2, t, 128), f32),
            pltpu.VMEM((d, t), f32),
            pltpu.VMEM((d, t), f32),
            pltpu.VMEM((d, t), f32),
            pltpu.VMEM((2, 4 * r, 4 * r), bf16),
            pltpu.VMEM((2, 4 * r, 4 * r), bf16),
            pltpu.VMEM((2, 4 * r, 4 * r), bf16),
            pltpu.VMEM((h, d, r), f32),
            pltpu.VMEM((h, d, r), f32),
            pltpu.VMEM((h, d, r), f32),
            pltpu.VMEM((h, 3, r, d), bf16),
            dma((3,)), dma((h,)), dma((h,)), dma((h,)),
            dma((3,)), dma((h,)), dma((h,)), dma((h,)),
            dma((3,)), dma((h,)), dma((h,)), dma((h,)),
            dma((2,)), dma((1,)),
        ],
        compiler_params=pltpu.CompilerParams(collective_id=0, has_side_effects=True, vmem_limit_bytes=63 * 1024 * 1024),
        name='attn_bwd',
    )(qh, doh, kh, vh, st)


def solution(mesh):
    fine = Mesh(mesh.devices.reshape((2,) * 7), AXES)
    rows = ('zh', 'zl', 'yh', 'yl', 'core', 'x1', 'x0')
    seq = P(None, rows, None, None)
    stat = P(None, None, rows)

    def body(q, k, v, o, do, lse):
        f32 = jnp.float32
        scale = q.shape[3] ** -0.5
        dlt = jnp.sum(do.astype(f32) * o.astype(f32), axis=-1)[0].T
        st = jnp.stack([lse[0], dlt], axis=1)
        grads = _attention(*[a[0].transpose(1, 0, 2) for a in (q, do, k, v)], st, scale)
        return tuple(g.transpose(1, 0, 2)[None] for g in grads)

    return jax.shard_map(body, mesh=fine, in_specs=(seq, seq, seq, seq, seq, stat), out_specs=(seq, seq, seq), check_vma=False)
```

```python
import functools

import jax
import jax.numpy as jnp
from jax import lax
from jax.experimental import pallas as pl
from jax.experimental.pallas import tpu as pltpu
from jax.sharding import Mesh, PartitionSpec as P

LOG2E = 1.4426950408889634
AXES = ('x1', 'x0', 'zh', 'zl', 'yh', 'yl', 'core')
N = 16
NA = 12
NF = 8
AHEAD = 1
FIRST = 4
NS = 3
LAG = 4


def _kernel(scale, qh, doh, kh, vh, st, out_q, out_k, out_v, qd, kv, qdt, kvt, sb, stb, dq, dkt, dvt, p_s, ds_s, dst_s, dq_rx, dk_rx, dv_rx, stage, send, recv_qd, recv_kv, recv_st, fwd_send, fwd_qd, fwd_kv, fwd_st, x_send, x_dq, x_dk, x_dv, o_send, o_recv):
    f32, bf16 = jnp.float32, jnp.bfloat16
    R = qh.shape[1]
    BT = 4 * R
    x1, x0, zh, zl, yh, yl, core = [lax.axis_index(a) for a in AXES]
    xb = (x0 + x1) % 2

    def source(m):
        a, b, c, d = m % 2, m // 2 % 2, m // 4 % 2, m // 8
        tx, ty, tzl, tzh = (a + b) % 2, (a + c) % 2, d, a
        sx = (x1 + tx) % 2
        return sx, (sx + xb) % 2, (zh + tzh) % 2, (zl + tzl) % 2, (yh + ty) % 2

    def device(m, u):
        sx, sx0, szh, szl, syh = source(m)
        return (sx, sx0, szh, szl, syh, (yl + u) % 2, core)

    def block(sx, syl):
        return syl + sx * (1 - 2 * syl)

    def place(m):
        sx, _, szh, szl, syh = source(m)
        zzy = 4 * szh + 2 * szl + syh
        return zzy + sx * (N - 1 - 2 * zzy)

    def head(dev):
        dx, _, dzh, dzl, dyh, dyl, _ = dev
        return (((dzh * 2 + dzl) * 2 + dyh) * 2 + dyl) * 2 + dx

    def chunk(m, b, i):
        return pl.ds(pl.multiple_of(m * BT + b * 2 * R + i * R, R), R)

    me = (x1, x0, zh, zl, yh, yl, core)
    x_peer = (x1, 1 - x0, zh, zl, yh, yl, core)
    c_peer = (x1, x0, zh, zl, yh, yl, 1 - core)
    my_b = block(x1, yl)

    def remote(src, dst, s_sem, r_sem, dev):
        return pltpu.make_async_remote_copy(src_ref=src, dst_ref=dst, send_sem=s_sem, recv_sem=r_sem, device_id=dev, device_id_type=pl.DeviceIdType.MESH)

    barrier = pltpu.get_barrier_semaphore()

    @pl.loop(1, 2 * N)
    def _(t):
        pl.semaphore_signal(barrier, inc=1, device_id=device(t // 2, t % 2), device_id_type=pl.DeviceIdType.MESH)

    for dev in (x_peer, c_peer):
        pl.semaphore_signal(barrier, inc=1, device_id=dev, device_id_type=pl.DeviceIdType.MESH)
    pl.semaphore_wait(barrier, 2 * N + 1)

    def parts(h, m, t):
        a, b = chunk(m, my_b, x0), chunk(m, my_b, core)
        return (
            (qh.at[h], qd.at[0, a, :], send.at[0], recv_qd.at[t]),
            (doh.at[h], qd.at[1, a, :], send.at[0], recv_qd.at[t]),
            (kh.at[h], kv.at[0, b, :], send.at[1], recv_kv.at[t]),
            (vh.at[h], kv.at[1, b, :], send.at[1], recv_kv.at[t]),
            (st.at[h], sb.at[:, a], send.at[2], recv_st.at[t]),
        )

    for src, dst, _, sem in parts(head(me), 0, 0):
        pltpu.make_async_copy(src, dst, sem).start()

    def issue(m):
        for u in range(2):
            @pl.when(2 * m + u > 0)
            def _():
                dev = device(m, u)
                for src, dst, ss, rs in parts(head(dev), m, 2 * m + u):
                    remote(src, dst, ss, rs, dev).start()

    @pl.loop(0, FIRST)
    def _(m):
        issue(m)

    def direct(m, u):
        sx, sx0, *_ = source(m)
        b = block(sx, (yl + u) % 2)
        return qd.at[:, chunk(m, b, sx0)], kv.at[:, chunk(m, b, core)], sb.at[:, chunk(m, b, sx0)]

    def passed(m, u):
        sx, sx0, *_ = source(m)
        b = block(sx, (yl + u) % 2)
        return qd.at[:, chunk(m, b, 1 - sx0)], kv.at[:, chunk(m, b, 1 - core)], sb.at[:, chunk(m, b, 1 - sx0)]

    def arrive(m):
        for u in range(2):
            t = 2 * m + u
            a, b, c = direct(m, u)
            pltpu.make_async_copy(a, a, recv_qd.at[t]).wait()
            remote(a, a, fwd_send.at[0], fwd_qd.at[t], x_peer).start()
            pltpu.make_async_copy(b, b, recv_kv.at[t]).wait()
            remote(b, b, fwd_send.at[1], fwd_kv.at[t], c_peer).start()
            pltpu.make_async_copy(c, c, recv_st.at[t]).wait()
            remote(c, c, fwd_send.at[2], fwd_st.at[t], x_peer).start()

        more = (m >= NS).astype(jnp.int32)
        w0 = FIRST + m + more * (m - NS)

        @pl.loop(w0, w0 + 1 + more)
        def _(w):
            @pl.when(w < N)
            def _():
                issue(w)

    def rows(i):
        return pl.ds(pl.multiple_of(i * BT, BT), BT)

    def complete(m):
        for u in range(2):
            t = 2 * m + u
            a, b, c = passed(m, u)
            pltpu.make_async_copy(a, a, fwd_qd.at[t]).wait()
            pltpu.make_async_copy(b, b, fwd_kv.at[t]).wait()
            pltpu.make_async_copy(c, c, fwd_st.at[t]).wait()
        rs = rows(m)
        for i in range(2):
            qdt[i, :, rs] = qd[i, rs, :].T
            kvt[i, :, rs] = kv[i, rs, :].T
        stb[0, rs, :] = jnp.broadcast_to(sb[0:1, rs] * LOG2E, (128, BT)).T
        stb[1, rs, :] = jnp.broadcast_to(sb[1:2, rs], (128, BT)).T

    dkt[...] = jnp.zeros_like(dkt)
    dvt[...] = jnp.zeros_like(dvt)
    dq[...] = jnp.zeros_like(dq)
    p_s[1] = jnp.zeros((BT, BT), bf16)
    ds_s[1] = jnp.zeros((BT, BT), bf16)
    dst_s[1] = jnp.zeros((BT, BT), bf16)

    def stage1(qb, kb, slot, diag):
        ks = rows(kb)
        for g in range(2):
            gs = pl.ds(pl.multiple_of(qb * BT + g * 2 * R, 2 * R), 2 * R)
            go = pl.ds(g * 2 * R, 2 * R)
            s = jnp.dot(qd[0, gs, :], kvt[0, :, ks], preferred_element_type=f32)
            dp = jnp.dot(qd[1, gs, :], kvt[1, :, ks], preferred_element_type=f32)
            lb, db = [jnp.tile(stb[i, gs, :], (1, BT // 128)) if BT >= 128 else stb[i, gs, :BT] for i in range(2)]
            p = jnp.exp2(s * (scale * LOG2E) - lb)
            if diag:
                hi = source(qb)[0]
                r = lax.broadcasted_iota(jnp.int32, p.shape, 0)
                c = lax.broadcasted_iota(jnp.int32, p.shape, 1)
                qp = (g * 2 + core + hi * (1 - 2 * core)) * (2 * R) + r
                cc = c // R % 2
                half = xb + hi * (1 - 2 * xb)
                kp = (c // (2 * R) * 2 + cc + hi * (1 - 2 * cc)) * (2 * R) + half * R + c % R
                p = jnp.where(kp <= qp, p, 0.0)
            p_s[slot, go, :] = p.astype(bf16)
            ds = (p * (dp - db)).astype(bf16)
            ds_s[slot, go, :] = ds
            dst_s[slot, :, go] = ds.T

    def stage2(qb, kb, slot):
        qs, ks = rows(qb), rows(kb)
        dvt[:, ks] += jnp.dot(qdt[1, :, qs], p_s[slot], preferred_element_type=f32)
        dkt[:, ks] += jnp.dot(qdt[0, :, qs], ds_s[slot], preferred_element_type=f32)
        dq[:, qs] += jnp.dot(kvt[0, :, ks], dst_s[slot], preferred_element_type=f32)

    def rank(i, j):
        late = (place(i) > place(j)).astype(jnp.int32)
        qb = j + late * (i - j)
        return qb, i + j - qb

    def two(i, j, carry):
        a, b = rank(i, j), rank(i, j + 1)
        stage2(*carry, 1)
        stage1(*a, 0, False)
        stage1(*b, 1, False)
        stage2(*a, 0)
        return b

    def four(i, j, carry, extra=lambda: None):
        a, b, c, d = [rank(i, j + n) for n in range(4)]
        stage2(*carry, 1)
        stage1(*a, 0, False)
        stage1(*b, 1, False)
        stage2(*a, 0)
        stage2(*b, 1)
        extra()
        stage1(*c, 0, False)
        stage1(*d, 1, False)
        stage2(*c, 0)
        return d

    def diagonal(i, j, with_pair, carry):
        @pl.when(with_pair)
        def _():
            a = rank(i, j)
            stage2(*carry, 1)
            stage1(*a, 0, False)
            stage1(i, i, 1, True)
            stage2(*a, 0)

        @pl.when(jnp.logical_not(with_pair))
        def _():
            stage2(*carry, 1)
            stage1(i, i, 1, True)

        return i, i

    def swap(m):
        sx, sx0, *_ = source(m)
        for b in range(2):
            w = 2 * m + b
            a = chunk(m, b, 1 - sx0)
            c = chunk(m, b, 1 - core)
            remote(dq.at[:, a], dq_rx.at[w], x_send.at[0], x_dq.at[w], x_peer).start()
            remote(dkt.at[:, c], dk_rx.at[w], x_send.at[1], x_dk.at[w], c_peer).start()
            remote(dvt.at[:, c], dv_rx.at[w], x_send.at[2], x_dv.at[w], c_peer).start()

    def swapped(m):
        for b in range(2):
            w = 2 * m + b
            for ref, sem in ((dq_rx, x_dq), (dk_rx, x_dk), (dv_rx, x_dv)):
                pltpu.make_async_copy(ref.at[w], ref.at[w], sem.at[w]).wait()

    def combine(m):
        sx, sx0, *_ = source(m)
        for b in range(2):
            w = 2 * m + b
            a = chunk(m, b, sx0)
            c = chunk(m, b, core)
            stage[w, 0] = ((dq[:, a] + dq_rx[w]) * scale).T.astype(bf16)
            stage[w, 1] = ((dkt[:, c] + dk_rx[w]) * scale).T.astype(bf16)
            stage[w, 2] = (dvt[:, c] + dv_rx[w]).T.astype(bf16)

    def emit(m):
        sx, sx0, szh, szl, syh = source(m)
        for b in range(2):
            syl = block(sx, b)
            dev = (sx, sx0, szh, szl, syh, syl, core)
            own = jnp.logical_and(m == 0, syl == yl)
            ends = [(stage.at[2 * m + b, i], o.at[head(me)]) for i, o in enumerate((out_q, out_k, out_v))]

            @pl.when(own)
            def _():
                for src, dst in ends:
                    pltpu.make_async_copy(src, dst, o_send.at[1]).start()

            @pl.when(jnp.logical_not(own))
            def _():
                for src, dst in ends:
                    remote(src, dst, o_send.at[0], o_recv.at[0], dev).start()

    @pl.loop(0, AHEAD)
    def _(m):
        arrive(m)

    def inflow(m, carry):
        count = 1 + (m >= NF).astype(jnp.int32)
        first = m + AHEAD + (m - NF) * (count - 1)

        @pl.loop(0, count)
        def _(i):
            @pl.when(first + i < N)
            def _():
                arrive(first + i)

        complete(m)
        j = m // 4 * 4
        some = m // 2 % 2 == 1

        @pl.when(some)
        def _():
            two(m, j, carry)

        carry = [jnp.where(some, a, b) for a, b in zip(rank(m, j + 1), carry)]
        carry = diagonal(m, m - 1, m % 2 == 1, carry)
        return lax.fori_loop(0, m // 4, lambda j, c: four(m, 4 * j, c), carry)

    carry = lax.fori_loop(0, NA, inflow, (0, 0))

    @pl.loop(NA, N)
    def _(m):
        complete(m)

    def outflow(f, carry):
        carry = four(f, NA, carry)

        @pl.when(f >= 1)
        def _():
            swap(f - 1)

        return carry

    def outflow_sums(f, carry):
        swapped(f - LAG)
        carry = four(f, NA, carry, lambda: combine(f - LAG))
        swap(f - 1)
        emit(f - LAG)
        return carry

    def finish(m):
        swapped(m)
        combine(m)
        emit(m)

    carry = lax.fori_loop(0, LAG, outflow, carry)
    carry = lax.fori_loop(LAG, NA, outflow_sums, carry)
    finish(NA - LAG)

    def last(f, carry):
        carry = diagonal(f, N - 1, f % 2 == 0, carry)
        swap(f - 1)
        carry = lax.fori_loop(0, (N - 1 - f) // 2, lambda j, c: two(f, f + 1 + 2 * j, c), carry)
        finish(f + 1 - LAG)
        return carry

    carry = lax.fori_loop(NA, N, last, carry)
    stage2(*carry, 1)
    swap(N - 1)

    @pl.loop(N + 1 - LAG, N)
    def _(m):
        finish(m)

    def drain(ref, sem):
        pltpu.make_async_copy(ref, ref, sem).wait()

    drain(stage.at[pl.ds(0, 2 * N - 1), pl.ds(0, 2)], send.at[0])
    drain(stage.at[pl.ds(0, 2 * N - 1), pl.ds(0, 2)], send.at[1])
    drain(st.at[pl.ds(0, 2 * N - 1)], send.at[2])
    drain(stage.at[pl.ds(0, 2 * N), pl.ds(0, 2)], fwd_send.at[0])
    drain(stage.at[pl.ds(0, 2 * N), pl.ds(0, 2)], fwd_send.at[1])
    drain(st.at[pl.ds(0, 2 * N)], fwd_send.at[2])
    drain(dq_rx, x_send.at[0])
    drain(dk_rx, x_send.at[1])
    drain(dv_rx, x_send.at[2])
    drain(stage.at[pl.ds(0, 2 * N - 1)], o_send.at[0])
    drain(stage.at[0], o_send.at[1])
    drain(stage.at[pl.ds(0, 2 * N - 1)], o_recv.at[0])


def _attention(qh, doh, kh, vh, st, scale):
    h, r, d = qh.shape
    t = 4 * r * N
    f32, bf16, dma = jnp.float32, jnp.bfloat16, pltpu.SemaphoreType.DMA
    hbm = pl.BlockSpec(memory_space=pl.ANY)
    return pl.pallas_call(
        functools.partial(_kernel, scale),
        out_shape=(jax.ShapeDtypeStruct((h, r, d), bf16),) * 3,
        in_specs=[hbm] * 5,
        out_specs=(hbm,) * 3,
        scratch_shapes=[
            pltpu.VMEM((2, t, d), bf16),
            pltpu.VMEM((2, t, d), bf16),
            pltpu.VMEM((2, d, t), bf16),
            pltpu.VMEM((2, d, t), bf16),
            pltpu.VMEM((2, t), f32),
            pltpu.VMEM((2, t, 128), f32),
            pltpu.VMEM((d, t), f32),
            pltpu.VMEM((d, t), f32),
            pltpu.VMEM((d, t), f32),
            pltpu.VMEM((2, 4 * r, 4 * r), bf16),
            pltpu.VMEM((2, 4 * r, 4 * r), bf16),
            pltpu.VMEM((2, 4 * r, 4 * r), bf16),
            pltpu.VMEM((h, d, r), f32),
            pltpu.VMEM((h, d, r), f32),
            pltpu.VMEM((h, d, r), f32),
            pltpu.VMEM((h, 3, r, d), bf16),
            dma((3,)), dma((h,)), dma((h,)), dma((h,)),
            dma((3,)), dma((h,)), dma((h,)), dma((h,)),
            dma((3,)), dma((h,)), dma((h,)), dma((h,)),
            dma((2,)), dma((1,)),
        ],
        compiler_params=pltpu.CompilerParams(collective_id=0, has_side_effects=True, vmem_limit_bytes=63 * 1024 * 1024),
        name='attn_bwd',
    )(qh, doh, kh, vh, st)


def solution(mesh):
    fine = Mesh(mesh.devices.reshape((2,) * 7), AXES)
    rows = ('zh', 'zl', 'yh', 'yl', 'core', 'x1', 'x0')
    seq = P(None, rows, None, None)
    stat = P(None, None, rows)

    def body(q, k, v, o, do, lse):
        f32 = jnp.float32
        scale = q.shape[3] ** -0.5
        dlt = jnp.sum(do.astype(f32) * o.astype(f32), axis=-1)[0].T
        st = jnp.stack([lse[0], dlt], axis=1)
        grads = _attention(*[a[0].transpose(1, 0, 2) for a in (q, do, k, v)], st, scale)
        return tuple(g.transpose(1, 0, 2)[None] for g in grads)

    return jax.shard_map(body, mesh=fine, in_specs=(seq, seq, seq, seq, seq, stat), out_specs=(seq, seq, seq), check_vma=False)
```

```python
import functools

import jax
import jax.numpy as jnp
from jax import lax
from jax.experimental import pallas as pl
from jax.experimental.pallas import tpu as pltpu
from jax.sharding import Mesh, PartitionSpec as P

LOG2E = 1.4426950408889634
AXES = ('x1', 'x0', 'zh', 'zl', 'yh', 'yl', 'core')
N = 16
NA = 12
NF = 8
AHEAD = 1
FIRST = 4
NS = 3
LAG = 4


def _kernel(scale, qh, doh, kh, vh, oh, lse, out_q, out_k, out_v, qd, kv, qdt, kvt, sb, stb, dq, dkt, dvt, p_s, ds_s, dst_s, dq_rx, dk_rx, dv_rx, stage, do_v, o_v, lse_v, st, load, send, recv_qd, recv_kv, recv_st, fwd_send, fwd_qd, fwd_kv, fwd_st, x_send, x_dq, x_dk, x_dv, o_send, o_recv):
    f32, bf16 = jnp.float32, jnp.bfloat16
    R = qh.shape[1]
    BT = 4 * R
    x1, x0, zh, zl, yh, yl, core = [lax.axis_index(a) for a in AXES]
    xb = (x0 + x1) % 2

    def source(m):
        a, b, c, d = m % 2, m // 2 % 2, m // 4 % 2, m // 8
        tx, ty, tzl, tzh = (a + b) % 2, (a + c) % 2, d, a
        sx = (x1 + tx) % 2
        return sx, (sx + xb) % 2, (zh + tzh) % 2, (zl + tzl) % 2, (yh + ty) % 2

    def device(m, u):
        sx, sx0, szh, szl, syh = source(m)
        return (sx, sx0, szh, szl, syh, (yl + u) % 2, core)

    def block(sx, syl):
        return syl + sx * (1 - 2 * syl)

    def place(m):
        sx, _, szh, szl, syh = source(m)
        zzy = 4 * szh + 2 * szl + syh
        return zzy + sx * (N - 1 - 2 * zzy)

    def head(dev):
        dx, _, dzh, dzl, dyh, dyl, _ = dev
        return (((dzh * 2 + dzl) * 2 + dyh) * 2 + dyl) * 2 + dx

    def chunk(m, b, i):
        return pl.ds(pl.multiple_of(m * BT + b * 2 * R + i * R, R), R)

    me = (x1, x0, zh, zl, yh, yl, core)
    x_peer = (x1, 1 - x0, zh, zl, yh, yl, core)
    c_peer = (x1, x0, zh, zl, yh, yl, 1 - core)
    my_b = block(x1, yl)

    def remote(src, dst, s_sem, r_sem, dev):
        return pltpu.make_async_remote_copy(src_ref=src, dst_ref=dst, send_sem=s_sem, recv_sem=r_sem, device_id=dev, device_id_type=pl.DeviceIdType.MESH)

    barrier = pltpu.get_barrier_semaphore()

    @pl.loop(1, 2 * N)
    def _(t):
        pl.semaphore_signal(barrier, inc=1, device_id=device(t // 2, t % 2), device_id_type=pl.DeviceIdType.MESH)

    for dev in (x_peer, c_peer):
        pl.semaphore_signal(barrier, inc=1, device_id=dev, device_id_type=pl.DeviceIdType.MESH)

    loads = [pltpu.make_async_copy(a, b, load.at[i]) for i, (a, b) in enumerate(((doh, do_v), (oh, o_v), (lse, lse_v)))]
    for c in loads:
        c.start()
    for c in loads:
        c.wait()

    @pl.loop(0, N)
    def _(n):
        for h in (2 * n, 2 * n + 1):
            e = do_v[h].astype(f32) * o_v[h].astype(f32)
            st[h, 0:1, :] = lse_v[pl.ds(h, 1), :]
            st[h, 1:2, :] = jnp.sum(e.T, axis=0, keepdims=True)

    pl.semaphore_wait(barrier, 2 * N + 1)

    def parts(h, m, t):
        a, b = chunk(m, my_b, x0), chunk(m, my_b, core)
        return (
            (qh.at[h], qd.at[0, a, :], send.at[0], recv_qd.at[t]),
            (doh.at[h], qd.at[1, a, :], send.at[0], recv_qd.at[t]),
            (kh.at[h], kv.at[0, b, :], send.at[1], recv_kv.at[t]),
            (vh.at[h], kv.at[1, b, :], send.at[1], recv_kv.at[t]),
            (st.at[h], sb.at[:, a], send.at[2], recv_st.at[t]),
        )

    for src, dst, _, sem in parts(head(me), 0, 0):
        pltpu.make_async_copy(src, dst, sem).start()

    def issue(m):
        for u in range(2):
            @pl.when(2 * m + u > 0)
            def _():
                dev = device(m, u)
                for src, dst, ss, rs in parts(head(dev), m, 2 * m + u):
                    remote(src, dst, ss, rs, dev).start()

    @pl.loop(0, FIRST)
    def _(m):
        issue(m)

    def direct(m, u):
        sx, sx0, *_ = source(m)
        b = block(sx, (yl + u) % 2)
        return qd.at[:, chunk(m, b, sx0)], kv.at[:, chunk(m, b, core)], sb.at[:, chunk(m, b, sx0)]

    def passed(m, u):
        sx, sx0, *_ = source(m)
        b = block(sx, (yl + u) % 2)
        return qd.at[:, chunk(m, b, 1 - sx0)], kv.at[:, chunk(m, b, 1 - core)], sb.at[:, chunk(m, b, 1 - sx0)]

    def arrive(m):
        for u in range(2):
            t = 2 * m + u
            a, b, c = direct(m, u)
            pltpu.make_async_copy(a, a, recv_qd.at[t]).wait()
            remote(a, a, fwd_send.at[0], fwd_qd.at[t], x_peer).start()
            pltpu.make_async_copy(b, b, recv_kv.at[t]).wait()
            remote(b, b, fwd_send.at[1], fwd_kv.at[t], c_peer).start()
            pltpu.make_async_copy(c, c, recv_st.at[t]).wait()
            remote(c, c, fwd_send.at[2], fwd_st.at[t], x_peer).start()

        more = (m >= NS).astype(jnp.int32)
        w0 = FIRST + m + more * (m - NS)

        @pl.loop(w0, w0 + 1 + more)
        def _(w):
            @pl.when(w < N)
            def _():
                issue(w)

    def rows(i):
        return pl.ds(pl.multiple_of(i * BT, BT), BT)

    def complete(m):
        for u in range(2):
            t = 2 * m + u
            a, b, c = passed(m, u)
            pltpu.make_async_copy(a, a, fwd_qd.at[t]).wait()
            pltpu.make_async_copy(b, b, fwd_kv.at[t]).wait()
            pltpu.make_async_copy(c, c, fwd_st.at[t]).wait()
        rs = rows(m)
        for i in range(2):
            qdt[i, :, rs] = qd[i, rs, :].T
            kvt[i, :, rs] = kv[i, rs, :].T
        stb[0, rs, :] = jnp.broadcast_to(sb[0:1, rs] * LOG2E, (128, BT)).T
        stb[1, rs, :] = jnp.broadcast_to(sb[1:2, rs], (128, BT)).T

    dkt[...] = jnp.zeros_like(dkt)
    dvt[...] = jnp.zeros_like(dvt)
    dq[...] = jnp.zeros_like(dq)
    p_s[1] = jnp.zeros((BT, BT), bf16)
    ds_s[1] = jnp.zeros((BT, BT), bf16)
    dst_s[1] = jnp.zeros((BT, BT), bf16)

    def stage1(qb, kb, slot, diag):
        ks = rows(kb)
        for g in range(2):
            gs = pl.ds(pl.multiple_of(qb * BT + g * 2 * R, 2 * R), 2 * R)
            go = pl.ds(g * 2 * R, 2 * R)
            s = jnp.dot(qd[0, gs, :], kvt[0, :, ks], preferred_element_type=f32)
            dp = jnp.dot(qd[1, gs, :], kvt[1, :, ks], preferred_element_type=f32)
            lb, db = [jnp.tile(stb[i, gs, :], (1, BT // 128)) if BT >= 128 else stb[i, gs, :BT] for i in range(2)]
            p = jnp.exp2(s * (scale * LOG2E) - lb)
            if diag:
                hi = source(qb)[0]
                r = lax.broadcasted_iota(jnp.int32, p.shape, 0)
                c = lax.broadcasted_iota(jnp.int32, p.shape, 1)
                qp = (g * 2 + core + hi * (1 - 2 * core)) * (2 * R) + r
                cc = c // R % 2
                half = xb + hi * (1 - 2 * xb)
                kp = (c // (2 * R) * 2 + cc + hi * (1 - 2 * cc)) * (2 * R) + half * R + c % R
                p = jnp.where(kp <= qp, p, 0.0)
            p_s[slot, go, :] = p.astype(bf16)
            ds = (p * (dp - db)).astype(bf16)
            ds_s[slot, go, :] = ds
            dst_s[slot, :, go] = ds.T

    def stage2(qb, kb, slot):
        qs, ks = rows(qb), rows(kb)
        dvt[:, ks] += jnp.dot(qdt[1, :, qs], p_s[slot], preferred_element_type=f32)
        dkt[:, ks] += jnp.dot(qdt[0, :, qs], ds_s[slot], preferred_element_type=f32)
        dq[:, qs] += jnp.dot(kvt[0, :, ks], dst_s[slot], preferred_element_type=f32)

    def rank(i, j):
        late = (place(i) > place(j)).astype(jnp.int32)
        qb = j + late * (i - j)
        return qb, i + j - qb

    def two(i, j, carry):
        a, b = rank(i, j), rank(i, j + 1)
        stage2(*carry, 1)
        stage1(*a, 0, False)
        stage1(*b, 1, False)
        stage2(*a, 0)
        return b

    def four(i, j, carry, extra=lambda: None):
        a, b, c, d = [rank(i, j + n) for n in range(4)]
        stage2(*carry, 1)
        stage1(*a, 0, False)
        stage1(*b, 1, False)
        stage2(*a, 0)
        stage2(*b, 1)
        extra()
        stage1(*c, 0, False)
        stage1(*d, 1, False)
        stage2(*c, 0)
        return d

    def diagonal(i, j, with_pair, carry):
        @pl.when(with_pair)
        def _():
            a = rank(i, j)
            stage2(*carry, 1)
            stage1(*a, 0, False)
            stage1(i, i, 1, True)
            stage2(*a, 0)

        @pl.when(jnp.logical_not(with_pair))
        def _():
            stage2(*carry, 1)
            stage1(i, i, 1, True)

        return i, i

    def swap(m):
        sx, sx0, *_ = source(m)
        for b in range(2):
            w = 2 * m + b
            a = chunk(m, b, 1 - sx0)
            c = chunk(m, b, 1 - core)
            remote(dq.at[:, a], dq_rx.at[w], x_send.at[0], x_dq.at[w], x_peer).start()
            remote(dkt.at[:, c], dk_rx.at[w], x_send.at[1], x_dk.at[w], c_peer).start()
            remote(dvt.at[:, c], dv_rx.at[w], x_send.at[2], x_dv.at[w], c_peer).start()

    def swapped(m):
        for b in range(2):
            w = 2 * m + b
            for ref, sem in ((dq_rx, x_dq), (dk_rx, x_dk), (dv_rx, x_dv)):
                pltpu.make_async_copy(ref.at[w], ref.at[w], sem.at[w]).wait()

    def combine(m):
        sx, sx0, *_ = source(m)
        for b in range(2):
            w = 2 * m + b
            a = chunk(m, b, sx0)
            c = chunk(m, b, core)
            stage[w, 0] = ((dq[:, a] + dq_rx[w]) * scale).T.astype(bf16)
            stage[w, 1] = ((dkt[:, c] + dk_rx[w]) * scale).T.astype(bf16)
            stage[w, 2] = (dvt[:, c] + dv_rx[w]).T.astype(bf16)

    def emit(m):
        sx, sx0, szh, szl, syh = source(m)
        for b in range(2):
            syl = block(sx, b)
            dev = (sx, sx0, szh, szl, syh, syl, core)
            own = jnp.logical_and(m == 0, syl == yl)
            ends = [(stage.at[2 * m + b, i], o.at[head(me)]) for i, o in enumerate((out_q, out_k, out_v))]

            @pl.when(own)
            def _():
                for src, dst in ends:
                    pltpu.make_async_copy(src, dst, o_send.at[1]).start()

            @pl.when(jnp.logical_not(own))
            def _():
                for src, dst in ends:
                    remote(src, dst, o_send.at[0], o_recv.at[0], dev).start()

    @pl.loop(0, AHEAD)
    def _(m):
        arrive(m)

    def inflow(m, carry):
        count = 1 + (m >= NF).astype(jnp.int32)
        first = m + AHEAD + (m - NF) * (count - 1)

        @pl.loop(0, count)
        def _(i):
            @pl.when(first + i < N)
            def _():
                arrive(first + i)

        complete(m)
        j = m // 4 * 4
        some = m // 2 % 2 == 1

        @pl.when(some)
        def _():
            two(m, j, carry)

        carry = [jnp.where(some, a, b) for a, b in zip(rank(m, j + 1), carry)]
        carry = diagonal(m, m - 1, m % 2 == 1, carry)
        return lax.fori_loop(0, m // 4, lambda j, c: four(m, 4 * j, c), carry)

    carry = lax.fori_loop(0, NA, inflow, (0, 0))

    @pl.loop(NA, N)
    def _(m):
        complete(m)

    def outflow(f, carry):
        carry = four(f, NA, carry)

        @pl.when(f >= 1)
        def _():
            swap(f - 1)

        return carry

    def outflow_sums(f, carry):
        swapped(f - LAG)
        carry = four(f, NA, carry, lambda: combine(f - LAG))
        swap(f - 1)
        emit(f - LAG)
        return carry

    def finish(m):
        swapped(m)
        combine(m)
        emit(m)

    carry = lax.fori_loop(0, LAG, outflow, carry)
    carry = lax.fori_loop(LAG, NA, outflow_sums, carry)
    finish(NA - LAG)

    def last(f, carry):
        carry = diagonal(f, N - 1, f % 2 == 0, carry)
        swap(f - 1)
        carry = lax.fori_loop(0, (N - 1 - f) // 2, lambda j, c: two(f, f + 1 + 2 * j, c), carry)
        finish(f + 1 - LAG)
        return carry

    carry = lax.fori_loop(NA, N, last, carry)
    stage2(*carry, 1)
    swap(N - 1)

    @pl.loop(N + 1 - LAG, N)
    def _(m):
        finish(m)

    def drain(ref, sem):
        pltpu.make_async_copy(ref, ref, sem).wait()

    drain(stage.at[pl.ds(0, 2 * N - 1), pl.ds(0, 2)], send.at[0])
    drain(stage.at[pl.ds(0, 2 * N - 1), pl.ds(0, 2)], send.at[1])
    drain(st.at[pl.ds(0, 2 * N - 1)], send.at[2])
    drain(stage.at[pl.ds(0, 2 * N), pl.ds(0, 2)], fwd_send.at[0])
    drain(stage.at[pl.ds(0, 2 * N), pl.ds(0, 2)], fwd_send.at[1])
    drain(st.at[pl.ds(0, 2 * N)], fwd_send.at[2])
    drain(dq_rx, x_send.at[0])
    drain(dk_rx, x_send.at[1])
    drain(dv_rx, x_send.at[2])
    drain(stage.at[pl.ds(0, 2 * N - 1)], o_send.at[0])
    drain(stage.at[0], o_send.at[1])
    drain(stage.at[pl.ds(0, 2 * N - 1)], o_recv.at[0])


def _attention(qh, doh, kh, vh, oh, lse, scale):
    h, r, d = qh.shape
    t = 4 * r * N
    f32, bf16, dma = jnp.float32, jnp.bfloat16, pltpu.SemaphoreType.DMA
    hbm = pl.BlockSpec(memory_space=pl.ANY)
    return pl.pallas_call(
        functools.partial(_kernel, scale),
        out_shape=(jax.ShapeDtypeStruct((h, r, d), bf16),) * 3,
        in_specs=[hbm] * 6,
        out_specs=(hbm,) * 3,
        scratch_shapes=[
            pltpu.VMEM((2, t, d), bf16),
            pltpu.VMEM((2, t, d), bf16),
            pltpu.VMEM((2, d, t), bf16),
            pltpu.VMEM((2, d, t), bf16),
            pltpu.VMEM((2, t), f32),
            pltpu.VMEM((2, t, 128), f32),
            pltpu.VMEM((d, t), f32),
            pltpu.VMEM((d, t), f32),
            pltpu.VMEM((d, t), f32),
            pltpu.VMEM((2, 4 * r, 4 * r), bf16),
            pltpu.VMEM((2, 4 * r, 4 * r), bf16),
            pltpu.VMEM((2, 4 * r, 4 * r), bf16),
            pltpu.VMEM((h, d, r), f32),
            pltpu.VMEM((h, d, r), f32),
            pltpu.VMEM((h, d, r), f32),
            pltpu.VMEM((h, 3, r, d), bf16),
            pltpu.VMEM((h, r, d), bf16),
            pltpu.VMEM((h, r, d), bf16),
            pltpu.VMEM((h, r), f32),
            pltpu.VMEM((h, 2, r), f32),
            dma((3,)),
            dma((3,)), dma((h,)), dma((h,)), dma((h,)),
            dma((3,)), dma((h,)), dma((h,)), dma((h,)),
            dma((3,)), dma((h,)), dma((h,)), dma((h,)),
            dma((2,)), dma((1,)),
        ],
        compiler_params=pltpu.CompilerParams(collective_id=0, has_side_effects=True, vmem_limit_bytes=63 * 1024 * 1024),
        name='attn_bwd',
    )(qh, doh, kh, vh, oh, lse)


def solution(mesh):
    fine = Mesh(mesh.devices.reshape((2,) * 7), AXES)
    rows = ('zh', 'zl', 'yh', 'yl', 'core', 'x1', 'x0')
    seq = P(None, rows, None, None)
    stat = P(None, None, rows)

    def body(q, k, v, o, do, lse):
        scale = q.shape[3] ** -0.5
        grads = _attention(*[a[0].transpose(1, 0, 2) for a in (q, do, k, v, o)], lse[0], scale)
        return tuple(g.transpose(1, 0, 2)[None] for g in grads)

    return jax.shard_map(body, mesh=fine, in_specs=(seq, seq, seq, seq, seq, stat), out_specs=(seq, seq, seq), check_vma=False)
```
